32 devices in a mesh: gx: 8 (over z, x), gz: 4 (over y, core).
Axes of the slice: x: 2, y: 2, z: 4, core: 2. Of those that a mesh axis runs over, the one named last changes fastest.
Arguments:
- velocity: float32 [3, 64, 128, 384], P(None, 'gx', 'gz'), may hold values from -6 to 6
- y_gap: float32 [385], replicated, may hold values from 0.2 to 2
Outputs:
- eddy_visc: float32 [64, 128, 384], P('gx', 'gz')
- lm_field: float32 [64, 128, 384], P('gx', 'gz')
- mm_field: float32 [64, 128, 384], P('gx', 'gz')
- coefficient: float32 [384], replicated
The draws below stay inside these ranges and needn't reach their ends.
All inputs are finite; a program needn't handle non-finite values.
Results may differ from the reference program's by a relative error of at most 0.00002.
Values sent between devices are 32-bit elements; how exact they have to be, the bound alone decides.
A program may use at most 64 MiB of HBM per device.

```python
import math
import jax
import jax.numpy as jnp
from jax import lax

NY = 384
NX = 64
NZ = 128


def block_levels(key, shape, split, smallest, top_value):
    gain, own = 1.0, jax.random.fold_in(key, 6)
    for dim, shards_of in split:
        draws = jnp.exp(jax.random.uniform(jax.random.fold_in(own, dim), (shards_of,), jnp.float32, smallest / len(split), top_value / len(split)))
        gain = gain * jnp.repeat(draws, shape[dim] // shards_of).reshape([-1 if axis == dim else 1 for axis in range(len(shape))])
    return gain


def scatter_about(stream_key, extent, spread, bound, cuts=(), held_as=jnp.bfloat16):
    entries = spread * jax.random.normal(stream_key, extent, jnp.float32)
    if cuts:
        entries = entries * block_levels(stream_key, extent, cuts, -0.22, 0.18)
    return jnp.clip(entries, -bound, bound).astype(held_as)


def setup_inputs(seed: int = 0) -> dict:
    arg_keys = jax.random.split(jax.random.key(seed), 3)
    velocity = scatter_about(arg_keys[0], (3, NX, NZ, NY), 1.0, 6.0, ((1, 8), (2, 4)), jnp.float32)
    y_gap = jnp.clip(jnp.exp(jax.random.uniform(arg_keys[1], (NY + 1,), jnp.float32, math.log(0.2), math.log(2.0))), 0.2, 2.0)
    return dict(velocity=velocity, y_gap=y_gap)


WEIGHTS = (1.0, 1.0, 1.0, 2.0, 2.0, 2.0)

def wall_slope(values, y_gap):
    padded = jnp.pad(values, [(0, 0)] * (values.ndim - 1) + [(1, 1)])
    return (padded[..., 2:] - padded[..., :-2]) / (y_gap[:-1] + y_gap[1:])

def strain_parts(slope_x, slope_y, slope_z):
    return jnp.stack([slope_x[0], slope_y[1], slope_z[2], 0.5 * (slope_y[0] + slope_x[1]), 0.5 * (slope_z[0] + slope_x[2]), 0.5 * (slope_z[1] + slope_y[2])])

def contract(first_part, second_part):
    summed = first_part[0] * second_part[0]
    for component in range(1, 6):
        summed = summed + WEIGHTS[component] * first_part[component] * second_part[component]
    return summed

def magnitude(strain):
    return jnp.sqrt(2.0 * contract(strain, strain))

def pair_products(speeds):
    return jnp.stack([speeds[0] * speeds[0], speeds[1] * speeds[1], speeds[2] * speeds[2], speeds[0] * speeds[1], speeds[0] * speeds[2], speeds[1] * speeds[2]])

def width_square(y_gap):
    return (0.5 * (y_gap[:-1] + y_gap[1:])) ** (2.0 / 3.0)

def germano(smooth_velocity, smooth_pairs, smooth_stress, test_strain, width_sq):
    leonard = smooth_pairs - pair_products(smooth_velocity)
    model_term = 2.0 * width_sq * (smooth_stress - 4.0 * magnitude(test_strain) * test_strain)
    return (contract(leonard, model_term), contract(model_term, model_term))

def periodic_strain(speeds, y_gap):
    slope_x = (jnp.roll(speeds, -1, 1) - jnp.roll(speeds, 1, 1)) * 0.5
    slope_z = (jnp.roll(speeds, -1, 2) - jnp.roll(speeds, 1, 2)) * 0.5
    slope_y = wall_slope(speeds, y_gap)
    return strain_parts(slope_x, slope_y, slope_z)

def periodic_filter(values):
    along_x = 0.25 * jnp.roll(values, 1, 1) + 0.5 * values + 0.25 * jnp.roll(values, -1, 1)
    return 0.25 * jnp.roll(along_x, 1, 2) + 0.5 * along_x + 0.25 * jnp.roll(along_x, -1, 2)

def reference(velocity, y_gap):
    width_sq = width_square(y_gap)
    strain = periodic_strain(velocity, y_gap)
    strain_size = magnitude(strain)
    smooth_velocity = periodic_filter(velocity)
    smooth_pairs = periodic_filter(pair_products(velocity))
    smooth_stress = periodic_filter(strain_size * strain)
    test_strain = periodic_strain(smooth_velocity, y_gap)
    lm_field, mm_field = germano(smooth_velocity, smooth_pairs, smooth_stress, test_strain, width_sq)
    planes = NX * NZ
    numerator = lax.optimization_barrier(jnp.sum(lm_field, axis=(0, 1)))
    denominator = lax.optimization_barrier(jnp.sum(mm_field, axis=(0, 1)))
    coefficient = numerator / planes / (denominator / planes + 1e-06)
    eddy_visc = coefficient * width_sq * strain_size
    return (eddy_visc, lm_field, mm_field, coefficient)
```

```python
import functools

import jax
import jax.numpy as jnp
from jax import lax
from jax.experimental import pallas as pl
from jax.experimental.pallas import tpu as pltpu
from jax.sharding import PartitionSpec as P

MESH = pl.DeviceIdType.MESH
LANES = 128
RIM = 8


def kernel(gxn, gzn, cells, coef_ref, vel_ref, eddy_ref, lm_ref, mm_ref, out_coef_ref,
           pad, zvel, zpair, zstress, slope, tslope, size_s, lm_s, mm_s, eddy_s, sums, acc_z, acc_x,
           local_sem, xs_sem, xr_sem, ks_sem, kr_sem, cs_sem, cr_sem,
           zs_sem, zr_sem, ws_sem, wr_sem, out_sem):
    gx, gz = lax.axis_index("gx"), lax.axis_index("gz")
    nx, nz, ny = vel_ref.shape[1:]
    wide = nz + RIM
    right, left = lax.rem(gx + 1, gxn), lax.rem(gx + gxn - 1, gxn)
    after, before = lax.rem(gz + 1, gzn), lax.rem(gz + gzn - 1, gzn)

    load = pltpu.make_async_copy(vel_ref, pad.at[:, 2:nx + 2, 0:nz], local_sem)
    load.start()
    barrier = pltpu.get_barrier_semaphore()
    for d in range(1, gxn):
        pl.semaphore_signal(barrier, inc=1, device_id=(lax.rem(gx + d, gxn), gz), device_id_type=MESH)
    for d in range(1, gzn):
        pl.semaphore_signal(barrier, inc=1, device_id=(gx, lax.rem(gz + d, gzn)), device_id_type=MESH)
    sums[...] = jnp.zeros_like(sums)
    load.wait()
    pl.semaphore_wait(barrier, gxn + gzn - 2)

    def remote(src, dst, send, recv, device):
        return pltpu.make_async_remote_copy(
            src_ref=src, dst_ref=dst, send_sem=send, recv_sem=recv,
            device_id=device, device_id_type=MESH)

    pieces = ((0, 8), (nz - 8, 8), (8, nz - 16))
    x_copies = []
    for n, (start, count) in enumerate(pieces):
        ks = pl.ds(start, count)
        x_copies.append((
            remote(pad.at[:, nx:nx + 2, ks], pad.at[:, 0:2, ks], xs_sem.at[n, 0], xr_sem.at[n, 0], (right, gz)),
            remote(pad.at[:, 2:4, ks], pad.at[:, nx + 2:nx + 4, ks], xs_sem.at[n, 1], xr_sem.at[n, 1], (left, gz))))
    k_up = remote(pad.at[:, 2:nx + 2, nz - 2:nz], pad.at[:, 2:nx + 2, wide - 2:wide], ks_sem.at[0], kr_sem.at[0], (gx, after))
    k_down = remote(pad.at[:, 2:nx + 2, 0:2], pad.at[:, 2:nx + 2, nz:nz + 2], ks_sem.at[1], kr_sem.at[1], (gx, before))
    k_up.start()
    k_down.start()
    for pair in x_copies:
        for copy in pair:
            copy.start()

    half_ahead, half_back = coef_ref[0:1, :], coef_ref[1:2, :]

    def filtered(f):
        twice = f + pltpu.roll(f, 1, 0)
        return twice + pltpu.roll(twice, wide - 1, 0)

    def lane_slope(f):
        return pltpu.roll(f, ny - 1, 1) * half_ahead - pltpu.roll(f, 1, 1) * half_back

    def tiles():
        return [pl.ds(t, LANES) for t in range(0, ny, LANES)]

    def smooth_row(r):
        for c in range(3):
            for cols in tiles():
                zvel[c, r, :, cols] = filtered(pad[c, r, :, cols])

    def first(r):
        for c in range(3):
            slope[c] = lane_slope(pad[c, r])
        for cols in tiles():
            u = [pad[c, r, :, cols] for c in range(3)]
            a = [pad[c, r + 1, :, cols] - pad[c, r - 1, :, cols] for c in range(3)]
            b = []
            for c in range(3):
                prev, nxt = pltpu.roll(u[c], 1, 0), pltpu.roll(u[c], wide - 1, 0)
                b.append(nxt - prev)
                zvel[c, r, :, cols] = (nxt + prev) + 2.0 * u[c]
            d = [slope[c, :, cols] for c in range(3)]
            strain = [a[0], d[1], b[2], d[0] + a[1], b[0] + a[2], b[1] + d[2]]
            square = [s * s for s in strain]
            size = jnp.sqrt(0.5 * (square[0] + square[1] + square[2]) + 0.25 * (square[3] + square[4] + square[5]))
            size_s[r, :, cols] = size[:nz]
            for n in range(6):
                zstress[n, r, :, cols] = filtered(size * strain[n])[:nz]
            for n, (i, j) in enumerate(((0, 0), (1, 1), (2, 2), (0, 1), (0, 2), (1, 2))):
                zpair[n, r, :, cols] = filtered(u[i] * u[j])[:nz]

    def second(r):
        for c in range(3):
            v = (zvel[c, r - 1] + zvel[c, r + 1]) + 2.0 * zvel[c, r]
            tslope[c] = v
            slope[c] = lane_slope(v)
        for cols in tiles():
            w = coef_ref[2:3, cols]
            w2 = coef_ref[3:4, cols]
            v_wide = [tslope[c, :, cols] for c in range(3)]
            v = [f[:nz] for f in v_wide]
            a = [(zvel[c, r + 2, 0:nz, cols] - zvel[c, r - 2, 0:nz, cols])
                 + 2.0 * (zvel[c, r + 1, 0:nz, cols] - zvel[c, r - 1, 0:nz, cols]) for c in range(3)]
            b = [(pltpu.roll(f, wide - 1, 0) - pltpu.roll(f, 1, 0))[:nz] for f in v_wide]
            d = [slope[c, 0:nz, cols] for c in range(3)]
            test = [a[0], d[1], b[2], d[0] + a[1], b[0] + a[2], b[1] + d[2]]
            square = [s * s for s in test]
            q = 0.25 * jnp.sqrt(0.5 * (square[0] + square[1] + square[2]) + 0.25 * (square[3] + square[4] + square[5]))
            lm, mm_diag, mm_off = 0.0, 0.0, 0.0
            for n, (i, j) in enumerate(((0, 0), (1, 1), (2, 2), (0, 1), (0, 2), (1, 2))):
                stress = (zstress[n, r - 1, :, cols] + zstress[n, r + 1, :, cols]) + 2.0 * zstress[n, r, :, cols]
                model = stress - q * test[n]
                pair = (zpair[n, r - 1, :, cols] + zpair[n, r + 1, :, cols]) + 2.0 * zpair[n, r, :, cols]
                lm = lm + (pair - v[i] * v[j] * 0.0625) * model
                if n < 3:
                    mm_diag = mm_diag + model * model
                else:
                    mm_off = mm_off + model * model
            lm = lm * w
            mm = (mm_diag + 0.5 * mm_off) * w2
            lm_s[r - 2, :, cols] = lm
            mm_s[r - 2, :, cols] = mm
            for n, f in enumerate((lm, mm)):
                sums[n, :, cols] += jnp.sum(f.reshape(nz // 8, 8, LANES), axis=0)

    def over(lo, hi, body):
        def step(r, carry):
            body(r)
            return carry
        lax.fori_loop(lo, hi, step, 0)

    k_up.wait_recv()
    k_down.wait_recv()
    over(3, nx + 1, first)
    for n in (0, 1):
        for copy in x_copies[n]:
            copy.wait_recv()
    corners = []
    for n, rows in enumerate((slice(0, 2), slice(nx + 2, nx + 4))):
        corners.append(remote(pad.at[:, rows, nz - 2:nz], pad.at[:, rows, wide - 2:wide], cs_sem.at[n, 0], cr_sem.at[n, 0], (gx, after)))
        corners.append(remote(pad.at[:, rows, 0:2], pad.at[:, rows, nz:nz + 2], cs_sem.at[n, 1], cr_sem.at[n, 1], (gx, before)))
    for copy in corners:
        copy.start()
    smooth_row(2)
    smooth_row(nx + 1)
    over(4, nx, second)
    for copy in x_copies[2]:
        copy.wait_recv()
    for copy in corners:
        copy.wait_recv()

    def edge(n, carry):
        first(lax.select(n < 2, n + 1, n + nx - 1))
        return carry

    def edge_second(n, carry):
        second(lax.select(n < 2, n + 2, n + nx - 2))
        return carry

    lax.fori_loop(0, 4, edge, 0)
    smooth_row(0)
    smooth_row(nx + 3)
    lax.fori_loop(0, 4, edge_second, 0)

    def exchange(acc, me, size, send, recv, device):
        copies = []
        for d in range(1, size):
            there = lax.rem(me + d, size)
            copy = remote(acc.at[me], acc.at[me], send.at[d - 1], recv.at[d - 1], device(there))
            copy.start()
            copies.append(copy)
        return copies

    def collect(acc, me, size, send, recv, device):
        for d in range(1, size):
            source = lax.rem(me + size - d, size)
            remote(acc.at[source], acc.at[source], send.at[d - 1], recv.at[d - 1], device(source)).wait_recv()
        total = acc[0]
        for n in range(1, size):
            total = total + acc[n]
        return total

    z_args = (acc_z, gz, gzn, zs_sem, zr_sem, lambda other: (gx, other))
    x_args = (acc_x, gx, gxn, ws_sem, wr_sem, lambda other: (other, gz))
    acc_z[gz] = jnp.sum(sums[...], axis=1)
    z_copies = exchange(*z_args)
    lm_out = pltpu.make_async_copy(lm_s, lm_ref, out_sem.at[0])
    mm_out = pltpu.make_async_copy(mm_s, mm_ref, out_sem.at[1])
    lm_out.start()
    mm_out.start()
    acc_x[gx] = collect(*z_args)
    w_copies = exchange(*x_args)
    total = collect(*x_args)
    coefficient = total[0:1] / cells / (total[1:2] / cells + 1e-06)
    out_coef_ref[...] = coefficient
    factor = coefficient * coef_ref[4:5, :]
    eddy_outs = []
    for r in range(nx):
        eddy_s[r] = factor * size_s[r + 2]
        copy = pltpu.make_async_copy(eddy_s.at[r], eddy_ref.at[r], out_sem.at[2 + r])
        copy.start()
        eddy_outs.append(copy)
    k_up.wait_send()
    k_down.wait_send()
    for pair in x_copies:
        for copy in pair:
            copy.wait_send()
    for copy in corners + z_copies + w_copies:
        copy.wait_send()
    lm_out.wait()
    mm_out.wait()
    for copy in eddy_outs:
        copy.wait()


def per_device(velocity, y_gap):
    gxn, gzn = lax.axis_size("gx"), lax.axis_size("gz")
    _, nx, nz, ny = velocity.shape
    cells = float(nx * gxn * nz * gzn)
    span = y_gap[:-1] + y_gap[1:]
    width_sq = (0.5 * span) ** (2.0 / 3.0)
    at = lax.iota(jnp.int32, ny)
    coefs = jnp.stack([
        jnp.where(at == ny - 1, 0.0, 2.0 / span),
        jnp.where(at == 0, 0.0, 2.0 / span),
        width_sq / 256.0,
        width_sq * width_sq / 256.0,
        width_sq, width_sq, width_sq, width_sq,
    ])
    field = jax.ShapeDtypeStruct((nx, nz, ny), jnp.float32)
    f32 = jnp.float32
    wide = nz + RIM
    dma = pltpu.SemaphoreType.DMA
    eddy, lm, mm, coefficient = pl.pallas_call(
        functools.partial(kernel, gxn, gzn, cells),
        out_shape=(field, field, field, jax.ShapeDtypeStruct((1, ny), f32)),
        in_specs=[pl.BlockSpec(memory_space=pltpu.VMEM), pl.BlockSpec(memory_space=pl.ANY)],
        out_specs=(pl.BlockSpec(memory_space=pl.ANY),) * 3 + (pl.BlockSpec(memory_space=pltpu.VMEM),),
        scratch_shapes=[
            pltpu.VMEM((3, nx + 4, wide, ny), f32),
            pltpu.VMEM((3, nx + 4, wide, ny), f32),
            pltpu.VMEM((6, nx + 4, nz, ny), f32),
            pltpu.VMEM((6, nx + 4, nz, ny), f32),
            pltpu.VMEM((3, wide, ny), f32),
            pltpu.VMEM((3, wide, ny), f32),
            pltpu.VMEM((nx + 4, nz, ny), f32),
            pltpu.VMEM((nx, nz, ny), f32),
            pltpu.VMEM((nx, nz, ny), f32),
            pltpu.VMEM((nx, nz, ny), f32),
            pltpu.VMEM((2, 8, ny), f32),
            pltpu.VMEM((gzn, 2, ny), f32),
            pltpu.VMEM((gxn, 2, ny), f32),
            dma, dma((3, 2)), dma((3, 2)), dma((2,)), dma((2,)), dma((2, 2)), dma((2, 2)),
            dma((max(gzn - 1, 1),)), dma((max(gzn - 1, 1),)), dma((max(gxn - 1, 1),)), dma((max(gxn - 1, 1),)),
            dma((2 + nx,)),
        ],
        compiler_params=pltpu.CompilerParams(collective_id=0, has_side_effects=True),
    )(coefs, velocity)
    return (eddy, lm, mm, coefficient.reshape(ny))


def solution(mesh):
    placed = (P(None, "gx", "gz", None), P())
    return jax.shard_map(
        per_device,
        mesh=mesh,
        in_specs=placed,
        out_specs=(P("gx", "gz", None), P("gx", "gz", None), P("gx", "gz", None), P()),
        check_vma=False,
    )
```

```python
import functools

import jax
import jax.numpy as jnp
from jax import lax
from jax.experimental import pallas as pl
from jax.experimental.pallas import tpu as pltpu
from jax.sharding import PartitionSpec as P

MESH = pl.DeviceIdType.MESH
LANES = 128
RIM = 8


def width_square(span):
    return jnp.exp(jnp.log(0.5 * span) * (2.0 / 3.0))


def finish(size_ref, lm_ref, mm_ref, coef_ref, gap_ref, eddy_out, lm_out, mm_out, coef_out, eddy_s, sem):
    nx, _, ny = size_ref.shape
    copies = [pltpu.make_async_copy(lm_ref, lm_out, sem.at[0]), pltpu.make_async_copy(mm_ref, mm_out, sem.at[1])]
    for copy in copies:
        copy.start()
    factor = coef_ref[...] * width_square(gap_ref[:, 0:ny] + gap_ref[:, 1:ny + 1])
    for r in range(0, nx, 2):
        rows = pl.ds(r, 2)
        eddy_s[rows] = factor * size_ref[rows]
        copy = pltpu.make_async_copy(eddy_s.at[rows], eddy_out.at[rows], sem.at[2 + r // 2])
        copy.start()
        copies.append(copy)
    coef_out[...] = coef_ref[...].reshape(ny)
    for copy in copies:
        copy.wait()


def kernel(gxn, gzn, cells, gap_ref, vel_ref, size_s, lm_s, mm_s, out_coef_ref,
           pad, zvel, zpair, zstress, slope, tslope, coef_ref, sums, acc_z, acc_x,
           local_sem, xs_sem, xr_sem, ks_sem, kr_sem, cs_sem, cr_sem,
           zs_sem, zr_sem, ws_sem, wr_sem):
    gx, gz = lax.axis_index("gx"), lax.axis_index("gz")
    nx, nz, ny = vel_ref.shape[1:]
    wide = nz + RIM
    right, left = lax.rem(gx + 1, gxn), lax.rem(gx + gxn - 1, gxn)
    after, before = lax.rem(gz + 1, gzn), lax.rem(gz + gzn - 1, gzn)

    load = pltpu.make_async_copy(vel_ref, pad.at[:, 2:nx + 2, 0:nz], local_sem)
    load.start()
    barrier = pltpu.get_barrier_semaphore()
    for d in range(1, gxn):
        pl.semaphore_signal(barrier, inc=1, device_id=(lax.rem(gx + d, gxn), gz), device_id_type=MESH)
    for d in range(1, gzn):
        pl.semaphore_signal(barrier, inc=1, device_id=(gx, lax.rem(gz + d, gzn)), device_id_type=MESH)
    sums[...] = jnp.zeros_like(sums)
    span = gap_ref[:, 0:ny] + gap_ref[:, 1:ny + 1]
    at = lax.broadcasted_iota(jnp.int32, (1, ny), 1)
    width_sq = width_square(span)
    inverse = 2.0 / span
    coef_ref[0:1] = jnp.where(at == ny - 1, 0.0, inverse)
    coef_ref[1:2] = jnp.where(at == 0, 0.0, inverse)
    coef_ref[2:3] = width_sq * (1.0 / 256.0)
    coef_ref[3:4] = width_sq * width_sq * (1.0 / 256.0)
    load.wait()
    pl.semaphore_wait(barrier, gxn + gzn - 2)

    def remote(src, dst, send, recv, device):
        return pltpu.make_async_remote_copy(
            src_ref=src, dst_ref=dst, send_sem=send, recv_sem=recv,
            device_id=device, device_id_type=MESH)

    pieces = ((1, 0, nz), (0, 0, 8), (0, nz - 8, 8), (0, 8, nz - 16))
    x_copies = []
    for n, (near, start, count) in enumerate(pieces):
        ks = pl.ds(start, count)
        low, high = near, 1 - near
        x_copies.append((
            remote(pad.at[:, nx + low, ks], pad.at[:, low, ks], xs_sem.at[n, 0], xr_sem.at[n, 0], (right, gz)),
            remote(pad.at[:, 2 + high, ks], pad.at[:, nx + 2 + high, ks], xs_sem.at[n, 1], xr_sem.at[n, 1], (left, gz))))
    k_up = remote(pad.at[:, 2:nx + 2, nz - 2:nz], pad.at[:, 2:nx + 2, wide - 2:wide], ks_sem.at[0], kr_sem.at[0], (gx, after))
    k_down = remote(pad.at[:, 2:nx + 2, 0:2], pad.at[:, 2:nx + 2, nz:nz + 2], ks_sem.at[1], kr_sem.at[1], (gx, before))
    k_up.start()
    k_down.start()
    for pair in x_copies:
        for copy in pair:
            copy.start()

    half_ahead, half_back = coef_ref[0:1, :], coef_ref[1:2, :]

    def filtered(f):
        twice = f + pltpu.roll(f, 1, 0)
        return twice + pltpu.roll(twice, wide - 1, 0)

    def lane_slope(f):
        return pltpu.roll(f, ny - 1, 1) * half_ahead - pltpu.roll(f, 1, 1) * half_back

    def tiles():
        return [pl.ds(t, LANES) for t in range(0, ny, LANES)]

    def smooth_row(r):
        for c in range(3):
            for cols in tiles():
                zvel[c, r, :, cols] = filtered(pad[c, r, :, cols])

    def first(r, inside=True):
        for c in range(3):
            slope[c] = lane_slope(pad[c, r])
        for cols in tiles():
            u = [pad[c, r, :, cols] for c in range(3)]
            a = [pad[c, r + 1, :, cols] - pad[c, r - 1, :, cols] for c in range(3)]
            b = []
            for c in range(3):
                prev, nxt = pltpu.roll(u[c], 1, 0), pltpu.roll(u[c], wide - 1, 0)
                b.append(nxt - prev)
                zvel[c, r, :, cols] = (nxt + prev) + 2.0 * u[c]
            d = [slope[c, :, cols] for c in range(3)]
            strain = [a[0], d[1], b[2], d[0] + a[1], b[0] + a[2], b[1] + d[2]]
            square = [s * s for s in strain]
            size = jnp.sqrt(0.5 * (square[0] + square[1] + square[2]) + 0.25 * (square[3] + square[4] + square[5]))
            if inside:
                size_s[r - 2, :, cols] = size[:nz]
            for n in range(6):
                zstress[n, r, :, cols] = filtered(size * strain[n])[:nz]
            for n, (i, j) in enumerate(((0, 0), (1, 1), (2, 2), (0, 1), (0, 2), (1, 2))):
                zpair[n, r, :, cols] = filtered(u[i] * u[j])[:nz]

    def second(r):
        for c in range(3):
            v = (zvel[c, r - 1] + zvel[c, r + 1]) + 2.0 * zvel[c, r]
            tslope[c] = v
            slope[c] = lane_slope(v)
        for cols in tiles():
            w = coef_ref[2:3, cols]
            w2 = coef_ref[3:4, cols]
            v_wide = [tslope[c, :, cols] for c in range(3)]
            v = [f[:nz] for f in v_wide]
            a = [(zvel[c, r + 2, 0:nz, cols] - zvel[c, r - 2, 0:nz, cols])
                 + 2.0 * (zvel[c, r + 1, 0:nz, cols] - zvel[c, r - 1, 0:nz, cols]) for c in range(3)]
            b = [(pltpu.roll(f, wide - 1, 0) - pltpu.roll(f, 1, 0))[:nz] for f in v_wide]
            d = [slope[c, 0:nz, cols] for c in range(3)]
            test = [a[0], d[1], b[2], d[0] + a[1], b[0] + a[2], b[1] + d[2]]
            square = [s * s for s in test]
            q = 0.25 * jnp.sqrt(0.5 * (square[0] + square[1] + square[2]) + 0.25 * (square[3] + square[4] + square[5]))
            lm, mm_diag, mm_off = 0.0, 0.0, 0.0
            for n, (i, j) in enumerate(((0, 0), (1, 1), (2, 2), (0, 1), (0, 2), (1, 2))):
                stress = (zstress[n, r - 1, :, cols] + zstress[n, r + 1, :, cols]) + 2.0 * zstress[n, r, :, cols]
                model = stress - q * test[n]
                pair = (zpair[n, r - 1, :, cols] + zpair[n, r + 1, :, cols]) + 2.0 * zpair[n, r, :, cols]
                lm = lm + (pair - v[i] * v[j] * 0.0625) * model
                if n < 3:
                    mm_diag = mm_diag + model * model
                else:
                    mm_off = mm_off + model * model
            lm = lm * w
            mm = (mm_diag + 0.5 * mm_off) * w2
            lm_s[r - 2, :, cols] = lm
            mm_s[r - 2, :, cols] = mm
            for n, f in enumerate((lm, mm)):
                sums[n, :, cols] += jnp.sum(f.reshape(nz // 8, 8, LANES), axis=0)

    def over(lo, hi, body):
        def step(r, carry):
            body(r)
            return carry
        lax.fori_loop(lo, hi, step, 0)

    k_up.wait_recv()
    k_down.wait_recv()
    over(3, nx + 1, first)
    smooth_row(2)
    smooth_row(nx + 1)
    over(4, nx, second)

    def pass_on(layer, low, high):
        copies = []
        for n, row in enumerate((low, high)):
            copies.append(remote(pad.at[:, row, nz - 2:nz], pad.at[:, row, wide - 2:wide], cs_sem.at[layer, n, 0], cr_sem.at[layer, n, 0], (gx, after)))
            copies.append(remote(pad.at[:, row, 0:2], pad.at[:, row, nz:nz + 2], cs_sem.at[layer, n, 1], cr_sem.at[layer, n, 1], (gx, before)))
        for copy in copies:
            copy.start()
        return copies

    def both(low, high, body):
        def step(n, carry):
            body(lax.select(n == 0, low, high))
            return carry
        lax.fori_loop(0, 2, step, 0)

    for copy in x_copies[0]:
        copy.wait_recv()
    corners = pass_on(0, 1, nx + 2)
    for copy in corners:
        copy.wait_recv()
    both(2, nx + 1, first)
    for n in (1, 2):
        for copy in x_copies[n]:
            copy.wait_recv()
    far = pass_on(1, 0, nx + 3)
    both(1, nx + 2, smooth_row)
    both(3, nx, second)
    for copy in far:
        copy.wait_recv()
    for copy in x_copies[3]:
        copy.wait_recv()
    corners = corners + far
    both(1, nx + 2, functools.partial(first, inside=False))
    both(0, nx + 3, smooth_row)
    both(2, nx + 1, second)

    def exchange(acc, me, size, send, recv, device):
        copies = []
        for d in range(1, size):
            there = lax.rem(me + d, size)
            copy = remote(acc.at[me], acc.at[me], send.at[d - 1], recv.at[d - 1], device(there))
            copy.start()
            copies.append(copy)
        return copies

    def collect(acc, me, size, send, recv, device):
        for d in range(1, size):
            source = lax.rem(me + size - d, size)
            remote(acc.at[source], acc.at[source], send.at[d - 1], recv.at[d - 1], device(source)).wait_recv()
        total = acc[0]
        for n in range(1, size):
            total = total + acc[n]
        return total

    z_args = (acc_z, gz, gzn, zs_sem, zr_sem, lambda other: (gx, other))
    x_args = (acc_x, gx, gxn, ws_sem, wr_sem, lambda other: (other, gz))
    acc_z[gz] = jnp.sum(sums[...], axis=1)
    z_copies = exchange(*z_args)
    acc_x[gx] = collect(*z_args)
    w_copies = exchange(*x_args)
    total = collect(*x_args)
    coefficient = total[0:1] / cells / (total[1:2] / cells + 1e-06)
    out_coef_ref[...] = coefficient
    k_up.wait_send()
    k_down.wait_send()
    for pair in x_copies:
        for copy in pair:
            copy.wait_send()
    for copy in corners + z_copies + w_copies:
        copy.wait_send()


def per_device(velocity, y_gap):
    gxn, gzn = lax.axis_size("gx"), lax.axis_size("gz")
    _, nx, nz, ny = velocity.shape
    cells = float(nx * gxn * nz * gzn)
    field = jax.ShapeDtypeStruct((nx, nz, ny), jnp.float32)
    f32 = jnp.float32
    wide = nz + RIM
    dma = pltpu.SemaphoreType.DMA
    gaps = y_gap.reshape(1, ny + 1)
    near = pl.BlockSpec(memory_space=pltpu.VMEM)
    far = pl.BlockSpec(memory_space=pl.ANY)
    held = pltpu.VMEM((nx, nz, ny), f32)
    size, lm, mm, coefficient = pl.pallas_call(
        functools.partial(kernel, gxn, gzn, cells),
        out_shape=(held, held, held, pltpu.VMEM((1, ny), f32)),
        in_specs=[near, far],
        out_specs=(near,) * 4,
        scratch_shapes=[
            pltpu.VMEM((3, nx + 4, wide, ny), f32),
            pltpu.VMEM((3, nx + 4, wide, ny), f32),
            pltpu.VMEM((6, nx + 4, nz, ny), f32),
            pltpu.VMEM((6, nx + 4, nz, ny), f32),
            pltpu.VMEM((3, wide, ny), f32),
            pltpu.VMEM((3, wide, ny), f32),
            pltpu.VMEM((8, ny), f32),
            pltpu.VMEM((2, 8, ny), f32),
            pltpu.VMEM((gzn, 2, ny), f32),
            pltpu.VMEM((gxn, 2, ny), f32),
            dma, dma((4, 2)), dma((4, 2)), dma((2,)), dma((2,)), dma((2, 2, 2)), dma((2, 2, 2)),
            dma((max(gzn - 1, 1),)), dma((max(gzn - 1, 1),)), dma((max(gxn - 1, 1),)), dma((max(gxn - 1, 1),)),
        ],
        compiler_params=pltpu.CompilerParams(
            collective_id=0, has_side_effects=True, vmem_limit_bytes=40 * 2**20),
    )(gaps, pltpu.with_memory_space_constraint(velocity, pltpu.HBM))
    return pl.pallas_call(
        finish,
        out_shape=(field, field, field, jax.ShapeDtypeStruct((ny,), f32)),
        in_specs=[near] * 5,
        out_specs=(far, far, far, near),
        scratch_shapes=[pltpu.VMEM((nx, nz, ny), f32), dma((2 + (nx + 1) // 2,))],
        compiler_params=pltpu.CompilerParams(vmem_limit_bytes=8 * 2**20),
    )(size, lm, mm, coefficient, gaps)


def solution(mesh):
    placed = (P(None, "gx", "gz", None), P())
    return jax.shard_map(
        per_device,
        mesh=mesh,
        in_specs=placed,
        out_specs=(P("gx", "gz", None), P("gx", "gz", None), P("gx", "gz", None), P()),
        check_vma=False,
    )
```

```python
import functools

import jax
import jax.numpy as jnp
from jax import lax
from jax.experimental import pallas as pl
from jax.experimental.pallas import tpu as pltpu
from jax.sharding import PartitionSpec as P

MESH = pl.DeviceIdType.MESH
LANES = 128
RIM = 8


def width_square(span):
    return jnp.exp(jnp.log(0.5 * span) * (2.0 / 3.0))


def finish(size_ref, lm_ref, mm_ref, coef_ref, eddy_out, lm_out, mm_out, coef_out, eddy_s, sem):
    nx, _, ny = size_ref.shape
    copies = [pltpu.make_async_copy(lm_ref, lm_out, sem.at[0]), pltpu.make_async_copy(mm_ref, mm_out, sem.at[1])]
    for copy in copies:
        copy.start()
    factor = coef_ref[1:2]
    for r in range(0, nx, 2):
        rows = pl.ds(r, 2)
        eddy_s[rows] = factor * size_ref[rows]
        copy = pltpu.make_async_copy(eddy_s.at[rows], eddy_out.at[rows], sem.at[2 + r // 2])
        copy.start()
        copies.append(copy)
    coef_out[...] = coef_ref[0:1].reshape(ny)
    for copy in copies:
        copy.wait()


def kernel(gxn, gzn, cells, gap_hbm, vel_ref, size_s, lm_s, mm_s, out_coef_ref,
           pad, zvel, zpair, zstress, slope, tslope, coef_ref, sums, acc_z, acc_x,
           gap_ref, gap_sem, local_sem, xs_sem, xr_sem, ks_sem, kr_sem, cs_sem, cr_sem,
           zs_sem, zr_sem, ws_sem, wr_sem):
    gx, gz = lax.axis_index("gx"), lax.axis_index("gz")
    nx, nz, ny = vel_ref.shape[1:]
    wide = nz + RIM
    right, left = lax.rem(gx + 1, gxn), lax.rem(gx + gxn - 1, gxn)
    after, before = lax.rem(gz + 1, gzn), lax.rem(gz + gzn - 1, gzn)

    load = pltpu.make_async_copy(vel_ref, pad.at[:, 2:nx + 2, 0:nz], local_sem)
    load.start()
    gap_load = pltpu.make_async_copy(gap_hbm, gap_ref, gap_sem)
    gap_load.start()
    barrier = pltpu.get_barrier_semaphore()
    for d in range(1, gxn):
        pl.semaphore_signal(barrier, inc=1, device_id=(lax.rem(gx + d, gxn), gz), device_id_type=MESH)
    for d in range(1, gzn):
        pl.semaphore_signal(barrier, inc=1, device_id=(gx, lax.rem(gz + d, gzn)), device_id_type=MESH)
    sums[...] = jnp.zeros_like(sums)
    gap_load.wait()
    span = gap_ref[:, 0:ny] + gap_ref[:, 1:ny + 1]
    at = lax.broadcasted_iota(jnp.int32, (1, ny), 1)
    width_sq = width_square(span)
    inverse = 2.0 / span
    coef_ref[0:1] = jnp.where(at == ny - 1, 0.0, inverse)
    coef_ref[1:2] = jnp.where(at == 0, 0.0, inverse)
    coef_ref[2:3] = width_sq * (1.0 / 256.0)
    coef_ref[3:4] = width_sq * width_sq * (1.0 / 256.0)
    coef_ref[4:5] = width_sq
    load.wait()
    pl.semaphore_wait(barrier, gxn + gzn - 2)

    def remote(src, dst, send, recv, device):
        return pltpu.make_async_remote_copy(
            src_ref=src, dst_ref=dst, send_sem=send, recv_sem=recv,
            device_id=device, device_id_type=MESH)

    pieces = ((slice(0, 2), 0, 8), (slice(0, 2), nz - 8, 8), (slice(1, 2), 8, nz - 16), (slice(0, 1), 8, nz - 16))
    x_copies = []
    for n, (layers, start, count) in enumerate(pieces):
        ks = pl.ds(start, count)
        low, high = layers.start, 2 - layers.stop
        deep = layers.stop - layers.start
        x_copies.append((
            remote(pad.at[:, nx + low:nx + low + deep, ks], pad.at[:, low:low + deep, ks], xs_sem.at[n, 0], xr_sem.at[n, 0], (right, gz)),
            remote(pad.at[:, 2 + high:2 + high + deep, ks], pad.at[:, nx + 2 + high:nx + 2 + high + deep, ks], xs_sem.at[n, 1], xr_sem.at[n, 1], (left, gz))))
    k_up = remote(pad.at[:, 2:nx + 2, nz - 2:nz], pad.at[:, 2:nx + 2, wide - 2:wide], ks_sem.at[0], kr_sem.at[0], (gx, after))
    k_down = remote(pad.at[:, 2:nx + 2, 0:2], pad.at[:, 2:nx + 2, nz:nz + 2], ks_sem.at[1], kr_sem.at[1], (gx, before))
    k_up.start()
    k_down.start()
    for pair in x_copies:
        for copy in pair:
            copy.start()

    half_ahead, half_back = coef_ref[0:1, :], coef_ref[1:2, :]

    def filtered(f):
        twice = f + pltpu.roll(f, 1, 0)
        return twice + pltpu.roll(twice, wide - 1, 0)

    def lane_slope(f):
        return pltpu.roll(f, ny - 1, 1) * half_ahead - pltpu.roll(f, 1, 1) * half_back

    def tiles():
        return [pl.ds(t, LANES) for t in range(0, ny, LANES)]

    def smooth_row(r):
        for c in range(3):
            for cols in tiles():
                zvel[c, r, :, cols] = filtered(pad[c, r, :, cols])

    def first(r, inside=True):
        for c in range(3):
            slope[c] = lane_slope(pad[c, r])
        for cols in tiles():
            u = [pad[c, r, :, cols] for c in range(3)]
            a = [pad[c, r + 1, :, cols] - pad[c, r - 1, :, cols] for c in range(3)]
            b = []
            for c in range(3):
                prev, nxt = pltpu.roll(u[c], 1, 0), pltpu.roll(u[c], wide - 1, 0)
                b.append(nxt - prev)
                zvel[c, r, :, cols] = (nxt + prev) + 2.0 * u[c]
            d = [slope[c, :, cols] for c in range(3)]
            strain = [a[0], d[1], b[2], d[0] + a[1], b[0] + a[2], b[1] + d[2]]
            square = [s * s for s in strain]
            size = jnp.sqrt(0.5 * (square[0] + square[1] + square[2]) + 0.25 * (square[3] + square[4] + square[5]))
            if inside:
                size_s[r - 2, :, cols] = size[:nz]
            for n in range(6):
                zstress[n, r, :, cols] = filtered(size * strain[n])[:nz]
            for n, (i, j) in enumerate(((0, 0), (1, 1), (2, 2), (0, 1), (0, 2), (1, 2))):
                zpair[n, r, :, cols] = filtered(u[i] * u[j])[:nz]

    def second(r):
        for c in range(3):
            v = (zvel[c, r - 1] + zvel[c, r + 1]) + 2.0 * zvel[c, r]
            tslope[c] = v
            slope[c] = lane_slope(v)
        for cols in tiles():
            w = coef_ref[2:3, cols]
            w2 = coef_ref[3:4, cols]
            v_wide = [tslope[c, :, cols] for c in range(3)]
            v = [f[:nz] for f in v_wide]
            a = [(zvel[c, r + 2, 0:nz, cols] - zvel[c, r - 2, 0:nz, cols])
                 + 2.0 * (zvel[c, r + 1, 0:nz, cols] - zvel[c, r - 1, 0:nz, cols]) for c in range(3)]
            b = [(pltpu.roll(f, wide - 1, 0) - pltpu.roll(f, 1, 0))[:nz] for f in v_wide]
            d = [slope[c, 0:nz, cols] for c in range(3)]
            test = [a[0], d[1], b[2], d[0] + a[1], b[0] + a[2], b[1] + d[2]]
            square = [s * s for s in test]
            q = 0.25 * jnp.sqrt(0.5 * (square[0] + square[1] + square[2]) + 0.25 * (square[3] + square[4] + square[5]))
            lm, mm_diag, mm_off = 0.0, 0.0, 0.0
            for n, (i, j) in enumerate(((0, 0), (1, 1), (2, 2), (0, 1), (0, 2), (1, 2))):
                stress = (zstress[n, r - 1, :, cols] + zstress[n, r + 1, :, cols]) + 2.0 * zstress[n, r, :, cols]
                model = stress - q * test[n]
                pair = (zpair[n, r - 1, :, cols] + zpair[n, r + 1, :, cols]) + 2.0 * zpair[n, r, :, cols]
                lm = lm + (pair - v[i] * v[j] * 0.0625) * model
                if n < 3:
                    mm_diag = mm_diag + model * model
                else:
                    mm_off = mm_off + model * model
            lm = lm * w
            mm = (mm_diag + 0.5 * mm_off) * w2
            lm_s[r - 2, :, cols] = lm
            mm_s[r - 2, :, cols] = mm
            for n, f in enumerate((lm, mm)):
                sums[n, :, cols] += jnp.sum(f.reshape(nz // 8, 8, LANES), axis=0)

    def over(lo, hi, body):
        def step(r, carry):
            body(r)
            return carry
        lax.fori_loop(lo, hi, step, 0)

    k_up.wait_recv()
    k_down.wait_recv()
    over(3, nx + 1, first)
    smooth_row(2)
    smooth_row(nx + 1)
    over(4, nx, second)

    def both(low, high, body):
        def step(n, carry):
            body(lax.select(n == 0, low, high))
            return carry
        lax.fori_loop(0, 2, step, 0)

    for n in (0, 1):
        for copy in x_copies[n]:
            copy.wait_recv()
    corners = []
    for n, rows in enumerate((slice(0, 2), slice(nx + 2, nx + 4))):
        corners.append(remote(pad.at[:, rows, nz - 2:nz], pad.at[:, rows, wide - 2:wide], cs_sem.at[n, 0], cr_sem.at[n, 0], (gx, after)))
        corners.append(remote(pad.at[:, rows, 0:2], pad.at[:, rows, nz:nz + 2], cs_sem.at[n, 1], cr_sem.at[n, 1], (gx, before)))
    for copy in corners:
        copy.start()
    for copy in x_copies[2]:
        copy.wait_recv()
    for copy in corners:
        copy.wait_recv()
    both(2, nx + 1, first)
    both(1, nx + 2, smooth_row)
    both(3, nx, second)
    for copy in x_copies[3]:
        copy.wait_recv()
    both(1, nx + 2, functools.partial(first, inside=False))
    both(0, nx + 3, smooth_row)
    both(2, nx + 1, second)

    def exchange(acc, me, size, send, recv, device):
        copies = []
        for d in range(1, size):
            there = lax.rem(me + d, size)
            copy = remote(acc.at[me], acc.at[me], send.at[d - 1], recv.at[d - 1], device(there))
            copy.start()
            copies.append(copy)
        return copies

    def collect(acc, me, size, send, recv, device):
        for d in range(1, size):
            source = lax.rem(me + size - d, size)
            remote(acc.at[source], acc.at[source], send.at[d - 1], recv.at[d - 1], device(source)).wait_recv()
        total = acc[0]
        for n in range(1, size):
            total = total + acc[n]
        return total

    z_args = (acc_z, gz, gzn, zs_sem, zr_sem, lambda other: (gx, other))
    x_args = (acc_x, gx, gxn, ws_sem, wr_sem, lambda other: (other, gz))
    acc_z[gz] = jnp.sum(sums[...], axis=1)
    z_copies = exchange(*z_args)
    acc_x[gx] = collect(*z_args)
    w_copies = exchange(*x_args)
    total = collect(*x_args)
    coefficient = total[0:1] / cells / (total[1:2] / cells + 1e-06)
    out_coef_ref[0:1] = coefficient
    out_coef_ref[1:2] = coefficient * coef_ref[4:5]
    k_up.wait_send()
    k_down.wait_send()
    for pair in x_copies:
        for copy in pair:
            copy.wait_send()
    for copy in corners + z_copies + w_copies:
        copy.wait_send()


def per_device(velocity, y_gap):
    gxn, gzn = lax.axis_size("gx"), lax.axis_size("gz")
    _, nx, nz, ny = velocity.shape
    cells = float(nx * gxn * nz * gzn)
    field = jax.ShapeDtypeStruct((nx, nz, ny), jnp.float32)
    f32 = jnp.float32
    wide = nz + RIM
    dma = pltpu.SemaphoreType.DMA
    gaps = y_gap.reshape(1, ny + 1)
    near = pl.BlockSpec(memory_space=pltpu.VMEM)
    far = pl.BlockSpec(memory_space=pl.ANY)
    held = pltpu.VMEM((nx, nz, ny), f32)
    size, lm, mm, coefficient = pl.pallas_call(
        functools.partial(kernel, gxn, gzn, cells),
        out_shape=(held, held, held, pltpu.VMEM((2, ny), f32)),
        in_specs=[far, far],
        out_specs=(near,) * 4,
        scratch_shapes=[
            pltpu.VMEM((3, nx + 4, wide, ny), f32),
            pltpu.VMEM((3, nx + 4, wide, ny), f32),
            pltpu.VMEM((6, nx + 4, nz, ny), f32),
            pltpu.VMEM((6, nx + 4, nz, ny), f32),
            pltpu.VMEM((3, wide, ny), f32),
            pltpu.VMEM((3, wide, ny), f32),
            pltpu.VMEM((8, ny), f32),
            pltpu.VMEM((2, 8, ny), f32),
            pltpu.VMEM((gzn, 2, ny), f32),
            pltpu.VMEM((gxn, 2, ny), f32),
            pltpu.VMEM((1, ny + 1), f32), dma,
            dma, dma((4, 2)), dma((4, 2)), dma((2,)), dma((2,)), dma((2, 2)), dma((2, 2)),
            dma((max(gzn - 1, 1),)), dma((max(gzn - 1, 1),)), dma((max(gxn - 1, 1),)), dma((max(gxn - 1, 1),)),
        ],
        compiler_params=pltpu.CompilerParams(
            collective_id=0, has_side_effects=True, vmem_limit_bytes=40 * 2**20),
    )(pltpu.with_memory_space_constraint(gaps, pltpu.HBM), pltpu.with_memory_space_constraint(velocity, pltpu.HBM))
    return pl.pallas_call(
        finish,
        out_shape=(field, field, field, jax.ShapeDtypeStruct((ny,), f32)),
        in_specs=[near] * 4,
        out_specs=(far, far, far, near),
        scratch_shapes=[pltpu.VMEM((nx, nz, ny), f32), dma((2 + (nx + 1) // 2,))],
        compiler_params=pltpu.CompilerParams(vmem_limit_bytes=8 * 2**20),
    )(size, lm, mm, coefficient)


def solution(mesh):
    placed = (P(None, "gx", "gz", None), P())
    return jax.shard_map(
        per_device,
        mesh=mesh,
        in_specs=placed,
        out_specs=(P("gx", "gz", None), P("gx", "gz", None), P("gx", "gz", None), P()),
        check_vma=False,
    )
```

```python
import functools

import jax
import jax.numpy as jnp
from jax import lax
from jax.experimental import pallas as pl
from jax.experimental.pallas import tpu as pltpu
from jax.sharding import PartitionSpec as P

MESH = pl.DeviceIdType.MESH
LANES = 128
RIM = 8


def width_square(span):
    return jnp.exp(jnp.log(0.5 * span) * (2.0 / 3.0))


def finish(size_ref, lm_ref, mm_ref, coef_ref, eddy_out, lm_out, mm_out, coef_out, eddy_s, sem):
    nx, _, ny = size_ref.shape
    copies = []
    for r in range(nx):
        copies.append(pltpu.make_async_copy(lm_ref.at[r], lm_out.at[r], sem.at[nx + r]))
        copies.append(pltpu.make_async_copy(mm_ref.at[r], mm_out.at[r], sem.at[2 * nx + r]))
    for copy in copies:
        copy.start()
    factor = coef_ref[1:2]
    for r in range(0, nx, 2):
        rows = pl.ds(r, 2)
        eddy_s[rows] = factor * size_ref[rows]
        copy = pltpu.make_async_copy(eddy_s.at[rows], eddy_out.at[rows], sem.at[r // 2])
        copy.start()
        copies.append(copy)
    coef_out[...] = coef_ref[0:1].reshape(ny)
    for copy in copies:
        copy.wait()


def kernel(gxn, gzn, cells, gap_hbm, vel_ref, size_s, lm_s, mm_s, out_coef_ref,
           pad, zvel, zpair, zstress, slope, tslope, coef_ref, sums, acc_z, acc_x,
           gap_ref, gap_sem, local_sem, xs_sem, xr_sem, ks_sem, kr_sem, cs_sem, cr_sem,
           zs_sem, zr_sem, ws_sem, wr_sem):
    gx, gz = lax.axis_index("gx"), lax.axis_index("gz")
    nx, nz, ny = vel_ref.shape[1:]
    wide = nz + RIM
    right, left = lax.rem(gx + 1, gxn), lax.rem(gx + gxn - 1, gxn)
    after, before = lax.rem(gz + 1, gzn), lax.rem(gz + gzn - 1, gzn)

    load = pltpu.make_async_copy(vel_ref, pad.at[:, 2:nx + 2, 0:nz], local_sem)
    load.start()
    gap_load = pltpu.make_async_copy(gap_hbm, gap_ref, gap_sem)
    gap_load.start()
    barrier = pltpu.get_barrier_semaphore()
    for d in sorted(range(1, gxn), key=lambda d: abs(2 * d - gxn)):
        pl.semaphore_signal(barrier, inc=1, device_id=(lax.rem(gx + d, gxn), gz), device_id_type=MESH)
    for d in range(1, gzn):
        pl.semaphore_signal(barrier, inc=1, device_id=(gx, lax.rem(gz + d, gzn)), device_id_type=MESH)
    sums[...] = jnp.zeros_like(sums)
    gap_load.wait()
    span = gap_ref[:, 0:ny] + gap_ref[:, 1:ny + 1]
    at = lax.broadcasted_iota(jnp.int32, (1, ny), 1)
    width_sq = width_square(span)
    inverse = 2.0 / span
    coef_ref[0:1] = jnp.where(at == ny - 1, 0.0, inverse)
    coef_ref[1:2] = jnp.where(at == 0, 0.0, inverse)
    coef_ref[2:3] = width_sq * (1.0 / 256.0)
    coef_ref[3:4] = width_sq * width_sq * (1.0 / 256.0)
    coef_ref[4:5] = width_sq
    load.wait()
    pl.semaphore_wait(barrier, gxn + gzn - 2)

    def remote(src, dst, send, recv, device):
        return pltpu.make_async_remote_copy(
            src_ref=src, dst_ref=dst, send_sem=send, recv_sem=recv,
            device_id=device, device_id_type=MESH)

    pieces = ((slice(0, 2), 0, 8), (slice(0, 2), nz - 8, 8), (slice(1, 2), 8, nz - 16), (slice(0, 1), 8, nz - 16))
    x_copies = []
    for n, (layers, start, count) in enumerate(pieces):
        ks = pl.ds(start, count)
        low, high = layers.start, 2 - layers.stop
        deep = layers.stop - layers.start
        x_copies.append((
            remote(pad.at[:, nx + low:nx + low + deep, ks], pad.at[:, low:low + deep, ks], xs_sem.at[n, 0], xr_sem.at[n, 0], (right, gz)),
            remote(pad.at[:, 2 + high:2 + high + deep, ks], pad.at[:, nx + 2 + high:nx + 2 + high + deep, ks], xs_sem.at[n, 1], xr_sem.at[n, 1], (left, gz))))
    k_up = remote(pad.at[:, 2:nx + 2, nz - 2:nz], pad.at[:, 2:nx + 2, wide - 2:wide], ks_sem.at[0], kr_sem.at[0], (gx, after))
    k_down = remote(pad.at[:, 2:nx + 2, 0:2], pad.at[:, 2:nx + 2, nz:nz + 2], ks_sem.at[1], kr_sem.at[1], (gx, before))
    k_up.start()
    k_down.start()
    for pair in x_copies:
        for copy in pair:
            copy.start()

    half_ahead, half_back = coef_ref[0:1, :], coef_ref[1:2, :]

    def filtered(f):
        twice = f + pltpu.roll(f, 1, 0)
        return twice + pltpu.roll(twice, wide - 1, 0)

    def lane_slope(f):
        return pltpu.roll(f, ny - 1, 1) * half_ahead - pltpu.roll(f, 1, 1) * half_back

    def tiles():
        return [pl.ds(t, LANES) for t in range(0, ny, LANES)]

    def smooth_row(r):
        for c in range(3):
            for cols in tiles():
                zvel[c, r, :, cols] = filtered(pad[c, r, :, cols])

    def first(r, inside=True):
        for c in range(3):
            slope[c] = lane_slope(pad[c, r])
        for cols in tiles():
            u = [pad[c, r, :, cols] for c in range(3)]
            a = [pad[c, r + 1, :, cols] - pad[c, r - 1, :, cols] for c in range(3)]
            b = []
            for c in range(3):
                prev, nxt = pltpu.roll(u[c], 1, 0), pltpu.roll(u[c], wide - 1, 0)
                b.append(nxt - prev)
                zvel[c, r, :, cols] = (nxt + prev) + 2.0 * u[c]
            d = [slope[c, :, cols] for c in range(3)]
            strain = [a[0], d[1], b[2], d[0] + a[1], b[0] + a[2], b[1] + d[2]]
            square = [s * s for s in strain]
            size = jnp.sqrt(0.5 * (square[0] + square[1] + square[2]) + 0.25 * (square[3] + square[4] + square[5]))
            if inside:
                size_s[r - 2, :, cols] = size[:nz]
            for n in range(6):
                zstress[n, r, :, cols] = filtered(size * strain[n])[:nz]
            for n, (i, j) in enumerate(((0, 0), (1, 1), (2, 2), (0, 1), (0, 2), (1, 2))):
                zpair[n, r, :, cols] = filtered(u[i] * u[j])[:nz]

    def second(r):
        for c in range(3):
            v = (zvel[c, r - 1] + zvel[c, r + 1]) + 2.0 * zvel[c, r]
            tslope[c] = v
            slope[c] = lane_slope(v)
        for cols in tiles():
            w = coef_ref[2:3, cols]
            w2 = coef_ref[3:4, cols]
            v_wide = [tslope[c, :, cols] for c in range(3)]
            v = [f[:nz] for f in v_wide]
            a = [(zvel[c, r + 2, 0:nz, cols] - zvel[c, r - 2, 0:nz, cols])
                 + 2.0 * (zvel[c, r + 1, 0:nz, cols] - zvel[c, r - 1, 0:nz, cols]) for c in range(3)]
            b = [(pltpu.roll(f, wide - 1, 0) - pltpu.roll(f, 1, 0))[:nz] for f in v_wide]
            d = [slope[c, 0:nz, cols] for c in range(3)]
            test = [a[0], d[1], b[2], d[0] + a[1], b[0] + a[2], b[1] + d[2]]
            square = [s * s for s in test]
            q = 0.25 * jnp.sqrt(0.5 * (square[0] + square[1] + square[2]) + 0.25 * (square[3] + square[4] + square[5]))
            lm, mm_diag, mm_off = 0.0, 0.0, 0.0
            for n, (i, j) in enumerate(((0, 0), (1, 1), (2, 2), (0, 1), (0, 2), (1, 2))):
                stress = (zstress[n, r - 1, :, cols] + zstress[n, r + 1, :, cols]) + 2.0 * zstress[n, r, :, cols]
                model = stress - q * test[n]
                pair = (zpair[n, r - 1, :, cols] + zpair[n, r + 1, :, cols]) + 2.0 * zpair[n, r, :, cols]
                lm = lm + (pair - v[i] * v[j] * 0.0625) * model
                if n < 3:
                    mm_diag = mm_diag + model * model
                else:
                    mm_off = mm_off + model * model
            lm = lm * w
            mm = (mm_diag + 0.5 * mm_off) * w2
            lm_s[r - 2, :, cols] = lm
            mm_s[r - 2, :, cols] = mm
            for n, f in enumerate((lm, mm)):
                sums[n, :, cols] += jnp.sum(f.reshape(nz // 8, 8, LANES), axis=0)

    def over(lo, hi, body):
        def step(r, carry):
            body(r)
            return carry
        lax.fori_loop(lo, hi, step, 0)

    k_up.wait_recv()
    k_down.wait_recv()
    over(3, nx + 1, first)
    smooth_row(2)
    smooth_row(nx + 1)
    over(4, nx, second)

    def both(low, high, body):
        def step(n, carry):
            body(lax.select(n == 0, low, high))
            return carry
        lax.fori_loop(0, 2, step, 0)

    for n in (0, 1):
        for copy in x_copies[n]:
            copy.wait_recv()
    corners = []
    for n, rows in enumerate((slice(0, 2), slice(nx + 2, nx + 4))):
        corners.append(remote(pad.at[:, rows, nz - 2:nz], pad.at[:, rows, wide - 2:wide], cs_sem.at[n, 0], cr_sem.at[n, 0], (gx, after)))
        corners.append(remote(pad.at[:, rows, 0:2], pad.at[:, rows, nz:nz + 2], cs_sem.at[n, 1], cr_sem.at[n, 1], (gx, before)))
    for copy in corners:
        copy.start()
    for copy in x_copies[2]:
        copy.wait_recv()
    for copy in corners:
        copy.wait_recv()
    both(2, nx + 1, first)
    both(1, nx + 2, smooth_row)
    both(3, nx, second)
    for copy in x_copies[3]:
        copy.wait_recv()
    both(1, nx + 2, functools.partial(first, inside=False))
    both(0, nx + 3, smooth_row)
    both(2, nx + 1, second)

    def exchange(acc, me, size, send, recv, device):
        copies = []
        for d in sorted(range(1, size), key=lambda d: abs(2 * d - size)):
            there = lax.rem(me + d, size)
            copy = remote(acc.at[me], acc.at[me], send.at[d - 1], recv.at[d - 1], device(there))
            copy.start()
            copies.append(copy)
        return copies

    def collect(acc, me, size, send, recv, device):
        for d in range(1, size):
            source = lax.rem(me + size - d, size)
            remote(acc.at[source], acc.at[source], send.at[d - 1], recv.at[d - 1], device(source)).wait_recv()
        total = acc[0]
        for n in range(1, size):
            total = total + acc[n]
        return total

    z_args = (acc_z, gz, gzn, zs_sem, zr_sem, lambda other: (gx, other))
    x_args = (acc_x, gx, gxn, ws_sem, wr_sem, lambda other: (other, gz))
    acc_z[gz] = jnp.sum(sums[...], axis=1)
    z_copies = exchange(*z_args)
    acc_x[gx] = collect(*z_args)
    w_copies = exchange(*x_args)
    total = collect(*x_args)
    coefficient = total[0:1] / cells / (total[1:2] / cells + 1e-06)
    out_coef_ref[0:1] = coefficient
    out_coef_ref[1:2] = coefficient * coef_ref[4:5]
    k_up.wait_send()
    k_down.wait_send()
    for pair in x_copies:
        for copy in pair:
            copy.wait_send()
    for copy in corners + z_copies + w_copies:
        copy.wait_send()


def per_device(velocity, y_gap):
    gxn, gzn = lax.axis_size("gx"), lax.axis_size("gz")
    _, nx, nz, ny = velocity.shape
    cells = float(nx * gxn * nz * gzn)
    field = jax.ShapeDtypeStruct((nx, nz, ny), jnp.float32)
    f32 = jnp.float32
    wide = nz + RIM
    dma = pltpu.SemaphoreType.DMA
    gaps = y_gap.reshape(1, ny + 1)
    near = pl.BlockSpec(memory_space=pltpu.VMEM)
    far = pl.BlockSpec(memory_space=pl.ANY)
    held = pltpu.VMEM((nx, nz, ny), f32)
    size, lm, mm, coefficient = pl.pallas_call(
        functools.partial(kernel, gxn, gzn, cells),
        out_shape=(held, held, held, pltpu.VMEM((2, ny), f32)),
        in_specs=[far, far],
        out_specs=(near,) * 4,
        scratch_shapes=[
            pltpu.VMEM((3, nx + 4, wide, ny), f32),
            pltpu.VMEM((3, nx + 4, wide, ny), f32),
            pltpu.VMEM((6, nx + 4, nz, ny), f32),
            pltpu.VMEM((6, nx + 4, nz, ny), f32),
            pltpu.VMEM((3, wide, ny), f32),
            pltpu.VMEM((3, wide, ny), f32),
            pltpu.VMEM((8, ny), f32),
            pltpu.VMEM((2, 8, ny), f32),
            pltpu.VMEM((gzn, 2, ny), f32),
            pltpu.VMEM((gxn, 2, ny), f32),
            pltpu.VMEM((1, ny + 1), f32), dma,
            dma, dma((4, 2)), dma((4, 2)), dma((2,)), dma((2,)), dma((2, 2)), dma((2, 2)),
            dma((max(gzn - 1, 1),)), dma((max(gzn - 1, 1),)), dma((max(gxn - 1, 1),)), dma((max(gxn - 1, 1),)),
        ],
        compiler_params=pltpu.CompilerParams(
            collective_id=0, has_side_effects=True, vmem_limit_bytes=40 * 2**20),
    )(pltpu.with_memory_space_constraint(gaps, pltpu.HBM), pltpu.with_memory_space_constraint(velocity, pltpu.HBM))
    return pl.pallas_call(
        finish,
        out_shape=(field, field, field, jax.ShapeDtypeStruct((ny,), f32)),
        in_specs=[near] * 4,
        out_specs=(far, far, far, near),
        scratch_shapes=[pltpu.VMEM((nx, nz, ny), f32), dma((3 * nx,))],
        compiler_params=pltpu.CompilerParams(vmem_limit_bytes=8 * 2**20),
    )(size, lm, mm, coefficient)


def solution(mesh):
    placed = (P(None, "gx", "gz", None), P())
    return jax.shard_map(
        per_device,
        mesh=mesh,
        in_specs=placed,
        out_specs=(P("gx", "gz", None), P("gx", "gz", None), P("gx", "gz", None), P()),
        check_vma=False,
    )
```
